256 devices in a mesh: rep: 2 (over core), dp: 128 (over x, y, z).
Axes of the slice: x: 4, y: 4, z: 8, core: 2. Of those that a mesh axis runs over, the one named last changes fastest.
Arguments:
- x: bfloat16 [256, 2048, 896], P(('rep', 'dp')), parts along dimension 0
- dy: bfloat16 [256, 2048, 896], P(('rep', 'dp')), parts along dimension 0
- w_gate: bfloat16 [2, 896, 2560], replicated
- w_up: bfloat16 [2, 896, 2560], replicated
- w_down: bfloat16 [2, 2560, 896], replicated
- m_w_gate: float32 [2, 896, 2560], replicated
- m_w_up: float32 [2, 896, 2560], replicated
- m_w_down: float32 [2, 2560, 896], replicated
- v_w_gate: float32 [2, 896, 2560], replicated
- v_w_up: float32 [2, 896, 2560], replicated
- v_w_down: float32 [2, 2560, 896], replicated
Outputs:
- output 1: bfloat16 [4, 896, 2560], P('rep'), parts along dimension 0
- output 2: bfloat16 [4, 896, 2560], P('rep'), parts along dimension 0
- output 3: bfloat16 [4, 2560, 896], P('rep'), parts along dimension 0
- output 4: float32 [4, 896, 2560], P('rep'), parts along dimension 0
- output 5: float32 [4, 896, 2560], P('rep'), parts along dimension 0
- output 6: float32 [4, 2560, 896], P('rep'), parts along dimension 0
- output 7: float32 [4, 896, 2560], P('rep'), parts along dimension 0
- output 8: float32 [4, 896, 2560], P('rep'), parts along dimension 0
- output 9: float32 [4, 2560, 896], P('rep'), parts along dimension 0
There are 2 independent parts. The reference program is written for one: setup_inputs(seed, part) draws one part's arguments, and reference() takes and returns one part's arrays. A program takes and returns all parts, laid end to end along the dimension named above; an argument that names none is the same for every part.
All inputs are finite; a program needn't handle non-finite values.
Results may differ from the reference program's by a relative error of at most 0.022.
Values are sent between devices in bfloat16 or wider.
A program may use at most 768 MiB of HBM per device.

```python
import jax
import jax.numpy as jnp
from jax import lax

SEQUENCES = 128
TOKENS = 2048
D = 896
FF = 2560
LAYERS = 2
NAMES = ("w_gate", "w_up", "w_down")
SHAPES = {"w_gate": (LAYERS, D, FF), "w_up": (LAYERS, D, FF), "w_down": (LAYERS, FF, D)}


def bump(key, n, height):
    away = (jnp.arange(n, dtype=jnp.int32) - jax.random.randint(key, (), 0, n, jnp.int32)) % n
    return jnp.where(away < n // 8, height, 1.0)


def together(key, own, strength):
    shared = jax.random.normal(key, own.shape[1:], jnp.float32)
    return (own + strength * shared) * lax.rsqrt(1 + strength * strength)


def setup_inputs(seed: int = 0, part: int = 0) -> dict:
    kx, kdy, ka, kb, kz, kf, kh, kl, *keys = jax.random.split(jax.random.key(seed), 8 + 3 * len(NAMES))
    kx, kdy, ka, kb = (jax.random.fold_in(k, part) for k in (kx, kdy, ka, kb))
    kw, km, kv = (keys[i::3] for i in range(3))
    shape = (SEQUENCES, TOKENS, D)
    much_x, much_dy = jax.random.uniform(kz, (2,), jnp.float32, 0.0, 1.0)
    loud = 2.0 ** jax.random.uniform(jax.random.fold_in(kz, 1), (), jnp.float32, -1.0, 2.0)
    layers = 2.0 ** jax.random.uniform(kl, (LAYERS, 1, 1), jnp.float32, -1.0, 1.0)
    x = together(ka, jax.random.normal(kx, shape, jnp.float32), much_x) * bump(kf, D, 4.0)
    dy = together(kb, jax.random.normal(kdy, shape, jnp.float32), much_dy)
    drawn = {"x": x.astype(jnp.bfloat16), "dy": (loud * dy * (SEQUENCES * TOKENS) ** -0.5).astype(jnp.bfloat16)}
    for key, name in zip(kw, NAMES, strict=True):
        w = jax.random.normal(key, SHAPES[name], jnp.float32) * SHAPES[name][1] ** -0.5
        drawn[name] = (w * {"w_gate": 1.0, "w_up": bump(kh, FF, 4.0), "w_down": layers}[name]).astype(jnp.bfloat16)
    for key, name in zip(km, NAMES, strict=True):
        drawn[f"m_{name}"] = 0.1 * jax.random.normal(key, SHAPES[name], jnp.float32)
    for key, name in zip(kv, NAMES, strict=True):
        drawn[f"v_{name}"] = jax.random.uniform(key, SHAPES[name], jnp.float32, 0.005, 0.015)
    return drawn


def matmul(a, w):
    return jnp.dot(a, w, preferred_element_type=jnp.float32).astype(jnp.bfloat16)


def normed(h):
    wide = h.astype(jnp.float32)
    scale = lax.rsqrt(jnp.mean(wide**2, -1, keepdims=True) + 1e-6)
    return (wide * scale).astype(jnp.bfloat16)


def layer(h, w):
    a = normed(h)
    gate = jnp.dot(a, w["w_gate"], preferred_element_type=jnp.float32)
    up = jnp.dot(a, w["w_up"], preferred_element_type=jnp.float32)
    return h + matmul((jax.nn.silu(gate) * up).astype(jnp.bfloat16), w["w_down"])


def adamw(w, m, v, g):
    m = 0.9 * m + 0.1 * g
    v = 0.95 * v + 0.05 * g * g
    step = m * lax.rsqrt(v + 1e-8) + 0.1 * w
    return (w - 0.02 * step).astype(jnp.bfloat16), m, v


def clipped(gradients, sum_of_squares, count):
    factor = jnp.minimum(1.0, 0.5 * lax.rsqrt(sum_of_squares / count + 1e-30))
    return [g * factor for g in gradients]


def stack(weights, h):
    return lax.scan(lambda h, w: (layer(h, w), None), h, weights)[0]


def reference(x, dy, w_gate, w_up, w_down, m_w_gate, m_w_up, m_w_down, v_w_gate, v_w_up, v_w_down):
    weights = dict(zip(NAMES, (w_gate, w_up, w_down), strict=True))

    def take(so_far, sequence):
        h, by_y = sequence
        _, back = jax.vjp(lambda w: stack(w, h), weights)
        return jax.tree.map(lambda total, term: total + term.astype(jnp.float32), so_far, back(by_y)[0]), None

    none_yet = {name: jnp.zeros(w.shape, jnp.float32) for name, w in weights.items()}
    by_weights, _ = lax.scan(take, none_yet, (x, dy))
    gradients = [by_weights[name].astype(jnp.bfloat16).astype(jnp.float32) for name in NAMES]
    gradients = clipped(gradients, sum(jnp.sum(g * g) for g in gradients), sum(g.size for g in gradients))
    new = [
        adamw(w.astype(jnp.float32), m, v, g)
        for w, m, v, g in zip((w_gate, w_up, w_down), (m_w_gate, m_w_up, m_w_down), (v_w_gate, v_w_up, v_w_down), gradients, strict=True)
    ]
    return tuple(one[which] for which in range(3) for one in new)
```

```python
import functools

import jax
import jax.numpy as jnp
from jax import lax
from jax.experimental import pallas as pl
from jax.experimental.pallas import tpu as pltpu
from jax.sharding import PartitionSpec as P

F32, BF16 = jnp.float32, jnp.bfloat16
S, D, FF = 2048, 896, 2560
MESH = pl.DeviceIdType.MESH
ANY = pl.BlockSpec(memory_space=pl.ANY)
TILE = (16, 128)
NT = 1152
SLAB = 384
SIZE = {"x": 4, "y": 4, "z": 8}
STRIDE = {"x": 32, "y": 8, "z": 1}
COLORS = (("x", "y", "z"), ("y", "x", "z"), ("z", "x", "y"))
RECV = 381
NN = (((1,), (0,)), ((), ()))
NT_ = (((1,), (1,)), ((), ()))
TN = (((0,), (0,)), ((), ()))


def dot(a, b, dims=NN):
    return lax.dot_general(a, b, dims, preferred_element_type=F32)


def norm_of(h):
    wide = h.astype(F32)
    return wide, lax.rsqrt(jnp.mean(wide * wide, -1, keepdims=True) + 1e-6)


def activations_kernel(CH, x_ref, dy_ref, wg_hbm, wu_hbm, wd_hbm, a0_ref, z0_ref, dg0_ref, du0_ref, a1_ref, z1_ref, dg1_ref, du1_ref, dh_ref, wg, wu, wd, gate0, up0, sem):
    first = pl.program_id(0) == 0
    n = FF // CH
    copies = [[pltpu.make_async_copy(hbm.at[layer], vmem.at[layer], sem.at[layer, k]) for k, (hbm, vmem) in enumerate(((wg_hbm, wg), (wu_hbm, wu), (wd_hbm, wd)))] for layer in range(2)]

    @pl.when(first)
    def _():
        for layer in range(2):
            for copy in copies[layer]:
                copy.start()
        copies[0][0].wait()
        copies[0][1].wait()

    x = x_ref[...]
    dy = dy_ref[...]
    wide, scale = norm_of(x)
    a = (wide * scale).astype(BF16)
    a0_ref[...] = a
    for j in range(n):
        at = pl.ds(j * CH, CH)
        gate, up = dot(a, wg[0, :, at]), dot(a, wu[0, :, at])
        gate0[:, at] = gate
        up0[:, at] = up
        z0_ref[:, at] = (gate * (0.5 + 0.5 * jnp.tanh(0.5 * gate)) * up).astype(BF16)

    @pl.when(first)
    def _():
        copies[0][2].wait()

    h = x + dot(z0_ref[...], wd[0]).astype(BF16)
    wide, scale = norm_of(h)
    a = (wide * scale).astype(BF16)
    a1_ref[...] = a

    @pl.when(first)
    def _():
        for copy in copies[1]:
            copy.wait()

    def back(gate, up, dz, dg_ref, du_ref, at):
        dz = dz.astype(BF16).astype(F32)
        sig = 0.5 + 0.5 * jnp.tanh(0.5 * gate)
        silu = gate * sig
        du_ref[:, at] = (dz * silu).astype(BF16)
        dg_ref[:, at] = (dz * up * (sig + silu * (1.0 - sig))).astype(BF16)
        return silu

    for j in range(n):
        at = pl.ds(j * CH, CH)
        gate, up, dz = dot(a, wg[1, :, at]), dot(a, wu[1, :, at]), dot(dy, wd[1, at, :], NT_)
        z1_ref[:, at] = (back(gate, up, dz, dg1_ref, du1_ref, at) * up).astype(BF16)
    da = (dot(dg1_ref[...], wg[1], NT_).astype(BF16) + dot(du1_ref[...], wu[1], NT_).astype(BF16)).astype(F32)
    by_mean = jnp.sum(da * wide, -1, keepdims=True) * (-1.0 / D) * (scale * scale * scale)
    dh = dy + (da * scale + by_mean * wide).astype(BF16)
    dh_ref[...] = dh
    for j in range(n):
        at = pl.ds(j * CH, CH)
        back(gate0[:, at], up0[:, at], dot(dh, wd[0, at, :], NT_), dg0_ref, du0_ref, at)


def activations(x, dy, w_gate, w_up, w_down, T=256, CH=512):
    row = lambda w: pl.BlockSpec((T, w), lambda i: (i, 0))
    widths = (D, FF, FF, FF, D, FF, FF, FF, D)
    return pl.pallas_call(
        functools.partial(activations_kernel, CH),
        name="activations",
        grid=(S // T,),
        in_specs=[row(D), row(D), ANY, ANY, ANY],
        out_specs=[row(w) for w in widths],
        out_shape=[jax.ShapeDtypeStruct((S, w), BF16) for w in widths],
        scratch_shapes=[pltpu.VMEM((2, D, FF), BF16), pltpu.VMEM((2, D, FF), BF16), pltpu.VMEM((2, FF, D), BF16), pltpu.VMEM((T, FF), F32), pltpu.VMEM((T, FF), F32),
                        pltpu.SemaphoreType.DMA((2, 3))],
        cost_estimate=pl.CostEstimate(flops=18 * S * D * FF, bytes_accessed=2 * S * (6 * FF + 5 * D) + 12 * D * FF, transcendentals=2 * S * FF),
        compiler_params=pltpu.CompilerParams(vmem_limit_bytes=63 * 2**20),
    )(x, dy, w_gate, w_up, w_down)


def adamw_kernel(transposed, k, ss_ref, g_ref, w_ref, m_ref, v_ref, wo, mo, vo):
    total = jnp.sum(ss_ref[...], keepdims=True)
    f = jnp.minimum(1.0, 0.5 * lax.rsqrt(total / (6 * D * FF) + 1e-30))
    def part(g, r, c):
        g = g.astype(F32) * f
        m = 0.9 * m_ref[0, r, c] + 0.1 * g
        v = 0.95 * v_ref[0, r, c] + 0.05 * g * g
        w = w_ref[0, r, c].astype(F32)
        mo[0, r, c] = m
        vo[0, r, c] = v
        wo[0, r, c] = (w - 0.02 * (m * lax.rsqrt(v + 1e-8) + 0.1 * w)).astype(BF16)
    if not transposed:
        @pl.loop(0, 56)
        def _(r):
            for j in range(k):
                part(g_ref[0, j * 56 + r], pl.ds(pl.multiple_of(r * 16, 16), 16), slice(j * 128, (j + 1) * 128))
    else:
        @pl.loop(0, 7)
        def _(r):
            for j in range(k):
                t = g_ref[0, pl.ds(j * 56 + r * 8, 8)].reshape(128, 128).T
                part(t, slice(j * 128, (j + 1) * 128), pl.ds(pl.multiple_of(r * 128, 128), 128))


def adamw(transposed, which, ss, g, w, m, v, k=5):
    if transposed:
        spec = pl.BlockSpec((1, 128 * k, D), lambda l, i: (l, i, 0))
    else:
        spec = pl.BlockSpec((1, D, 128 * k), lambda l, i: (l, 0, i))
    gspec = pl.BlockSpec((1, 56 * k, 16, 128), lambda l, i: (which - 3 * l, i, 0, 0))
    n = w.size
    return pl.pallas_call(functools.partial(adamw_kernel, transposed, k), name="adamw", grid=(2, 20 // k),
        in_specs=[pl.BlockSpec((8, 128), lambda l, i: (0, 0)), gspec, spec, spec, spec], out_specs=[spec] * 3,
        out_shape=[jax.ShapeDtypeStruct(w.shape, BF16), jax.ShapeDtypeStruct(w.shape, F32), jax.ShapeDtypeStruct(w.shape, F32)],
        cost_estimate=pl.CostEstimate(flops=20 * n, bytes_accessed=22 * n, transcendentals=n),
        compiler_params=pltpu.CompilerParams(vmem_limit_bytes=48 * 2**20))(ss, g, w, m, v)


class Geo:
    def __init__(self, c):
        self.c = c
        self.p, self.q, self.r = COLORS[c]
        self.n, self.nq, self.nr = (SIZE[a] for a in COLORS[c])
        self.h = self.n // 2
        self.C = SLAB // self.n
        self.H = self.C // 2
        self.Cq = self.C // self.nq
        assert self.Cq == 3 * self.nr
        self.own = 2 * self.H + 2 * self.C * (self.h - 2) + self.C
        self.p2 = 2 * self.H + 2 * self.C * (self.h - 1)
        self.p3 = self.p2 + (self.nq - 1) * self.Cq
        assert self.p3 + 3 * (self.nr - 1) == RECV

    def L(self, s):
        return 2 * self.H + (s - 2) * 2 * self.C

    def R(self, s):
        return self.L(s) + self.C

    def own_step(self, s):
        return 2 * self.H + (s - 3) * 2 * self.C

    @property
    def own_mine(self):
        return 2 * self.H + 2 * self.C * (self.h - 2)


GEO = [Geo(c) for c in range(3)]
OWN = max(g.own for g in GEO)
RING = 4


def add_loop(n, body, unroll):
    assert n % unroll == 0
    if n == unroll:
        body(0, unroll)
    else:
        pl.loop(0, n // unroll)(lambda i: body(i * unroll, unroll))


class Comm:
    def __init__(self, g, out, recv, own, own1, own2, fin, sems):
        self.g, self.out, self.recv, self.own, self.own1, self.own2, self.fin = g, out, recv, own, own1, own2, fin
        (self.s_rs, self.s_ag, self.s_own, self.s_a, self.s_b, self.s_l, self.s_r, self.s_p2, self.s_p3, self.s_loc,
         self.s_gr, self.s_gq, self.s_gl, self.s_gright) = sems
        me = lax.axis_index("dp")
        self.me = me
        self.at = {"x": me // 32, "y": me // 8 % 4, "z": me % 8}

    def shift(self, ax, d):
        return lax.rem(self.at[ax] + (d + SIZE[ax]), SIZE[ax])

    def peer(self, ax, d):
        return {"dp": self.me + (self.shift(ax, d) - self.at[ax]) * STRIDE[ax]}

    def barrier(self):
        b = pltpu.get_barrier_semaphore()
        count = 0
        for ax in "xyz":
            for d in range(1, SIZE[ax]):
                pl.semaphore_signal(b, inc=1, device_id=self.peer(ax, d), device_id_type=MESH)
                count += 1
        pl.semaphore_wait(b, count)

    def send(self, src, dst, ssem, rsem, ax, d):
        pltpu.make_async_remote_copy(src_ref=src, dst_ref=dst, send_sem=ssem, recv_sem=rsem, device_id=self.peer(ax, d), device_id_type=MESH).start()

    def wait(self, ref, n, sem):
        pltpu.make_async_copy(ref.at[pl.ds(0, n)], ref.at[pl.ds(0, n)], sem).wait()

    def got(self, m, c, n, sem):
        self.wait(self.recv.at[m, c], n, sem)

    def raw(self, m, c):
        G = GEO[c]
        g, rv = self.g.at[m], self.recv.at[m, c]
        chunk = lambda d: c * SLAB + self.shift(G.p, d) * G.C
        ss = self.s_rs.at[m, c]
        self.send(g.at[pl.ds(chunk(G.h), G.H)], rv.at[pl.ds(0, G.H)], ss, self.s_a.at[m, c], G.p, 1)
        self.send(g.at[pl.ds(chunk(G.h) + G.H, G.H)], rv.at[pl.ds(G.H, G.H)], ss, self.s_b.at[m, c], G.p, -1)
        self.send(g.at[pl.ds(chunk(G.h - 1) + G.H, G.H)], rv.at[pl.ds(G.L(2) + G.H, G.H)], ss, self.s_l.at[m, c, 0], G.p, 1)
        self.send(g.at[pl.ds(chunk(1 - G.h), G.H)], rv.at[pl.ds(G.R(2), G.H)], ss, self.s_r.at[m, c, 0], G.p, -1)

    def load(self, m, c):
        G = GEO[c]
        g, own = self.g.at[m], self.own.at[m % RING, c]
        chunk = lambda d: c * SLAB + self.shift(G.p, d) * G.C
        parts = [(chunk(G.h - 1), 0, G.H), (chunk(1 - G.h) + G.H, G.H, G.H)]
        for s in range(3, G.h + 1):
            parts += [(chunk(G.h - s + 1), G.own_step(s), G.C), (chunk(s - G.h - 1), G.own_step(s) + G.C, G.C)]
        parts += [(chunk(0), G.own_mine, G.C)]
        for src, dst, n in parts:
            pltpu.make_async_copy(g.at[pl.ds(src, n)], own.at[pl.ds(dst, n)], self.s_own.at[m, c]).start()

    def add_in(self, m, c, at, own_at, n):
        rv, own = self.recv.at[m, c], self.own.at[m % RING, c]

        def body(i, k):
            rv[pl.ds(at + i, k)] = (rv[pl.ds(at + i, k)].astype(F32) + own[pl.ds(own_at + i, k)].astype(F32)).astype(BF16)

        add_loop(n, body, 8)

    def step(self, m, c, s):
        G = GEO[c]
        rv = self.recv.at[m, c]
        ss = self.s_rs.at[m, c]
        if s == 2:
            self.wait(self.own.at[m % RING, c], G.own, self.s_own.at[m, c])
            self.got(m, c, G.H, self.s_a.at[m, c])
            self.add_in(m, c, 0, 0, G.H)
            self.got(m, c, G.H, self.s_b.at[m, c])
            self.send(rv.at[pl.ds(0, G.H)], rv.at[pl.ds(G.L(2), G.H)], ss, self.s_l.at[m, c, 0], G.p, 1)
            self.add_in(m, c, G.H, G.H, G.H)
            self.send(rv.at[pl.ds(G.H, G.H)], rv.at[pl.ds(G.R(2) + G.H, G.H)], ss, self.s_r.at[m, c, 0], G.p, -1)
        else:
            self.got(m, c, G.C, self.s_l.at[m, c, s - 3])
            self.add_in(m, c, G.L(s - 1), G.own_step(s), G.C)
            self.got(m, c, G.C, self.s_r.at[m, c, s - 3])
            self.send(rv.at[pl.ds(G.L(s - 1), G.C)], rv.at[pl.ds(G.L(s), G.C)], ss, self.s_l.at[m, c, s - 2], G.p, 1)
            self.add_in(m, c, G.R(s - 1), G.own_step(s) + G.C, G.C)
            self.send(rv.at[pl.ds(G.R(s - 1), G.C)], rv.at[pl.ds(G.R(s), G.C)], ss, self.s_r.at[m, c, s - 2], G.p, -1)

    def first(self, m, c):
        G = GEO[c]
        rv, own = self.recv.at[m, c], self.own.at[m % RING, c]
        l, r, mine = G.L(G.h), G.R(G.h), G.own_mine
        self.got(m, c, G.C, self.s_l.at[m, c, G.h - 2])
        self.got(m, c, G.C, self.s_r.at[m, c, G.h - 2])

        def total(i, k):
            return own[pl.ds(mine + i, k)].astype(F32) + rv[pl.ds(l + i, k)].astype(F32) + rv[pl.ds(r + i, k)].astype(F32)

        keep = self.at[G.q] * G.Cq

        def body0(i, k):
            self.own1[m % RING, c, pl.ds(i, k)] = total(keep + i, k)

        def body1(i, k):
            rv[pl.ds(l + i, k)] = total(i, k).astype(BF16)

        add_loop(G.Cq, body0, 4)
        add_loop(G.C, body1, 8)
        for d in range(1, G.nq):
            self.send(rv.at[pl.ds(l + self.shift(G.q, d) * G.Cq, G.Cq)], rv.at[pl.ds(G.p2 + (d - 1) * G.Cq, G.Cq)],
                      self.s_rs.at[m, c], self.s_p2.at[m, c], G.q, d)

    def second(self, m, c):
        G = GEO[c]
        rv = self.recv.at[m, c]
        self.got(m, c, (G.nq - 1) * G.Cq, self.s_p2.at[m, c])

        def total(i, k):
            t = self.own1[m % RING, c, pl.ds(i, k)]
            for d in range(G.nq - 1):
                t = t + rv[pl.ds(G.p2 + d * G.Cq + i, k)].astype(F32)
            return t

        self.own2[m % RING, c] = total(self.at[G.r] * 3, 3)

        def body(i, k):
            rv[pl.ds(G.p2 + i, k)] = total(i, k).astype(BF16)

        add_loop(G.Cq, body, 4)
        for d in range(1, G.nr):
            self.send(rv.at[pl.ds(G.p2 + self.shift(G.r, d) * 3, 3)], rv.at[pl.ds(G.p3 + (d - 1) * 3, 3)],
                      self.s_rs.at[m, c], self.s_p3.at[m, c], G.r, d)

    def third(self, m, c):
        G = GEO[c]
        rv = self.recv.at[m, c]
        self.got(m, c, (G.nr - 1) * 3, self.s_p3.at[m, c])
        t = self.own2[m % RING, c]
        for d in range(G.nr - 1):
            t = t + rv[pl.ds(G.p3 + 3 * d, 3)].astype(F32)
        t = t.astype(BF16)
        self.fin[m, c] = t
        t = t.astype(F32)
        return jnp.sum((t * t).reshape(6, 8, 128), axis=0)

    def rs_sent(self, m, c):
        G = GEO[c]
        n = 4 * G.H + 2 * G.H + 2 * G.C * (G.h - 2) + (G.nq - 1) * G.Cq + (G.nr - 1) * 3
        self.wait(self.g.at[m], n, self.s_rs.at[m, c])

    def place(self, c, p, q=None, r=None):
        G = GEO[c]
        return c * SLAB + p * G.C + (0 if q is None else q * G.Cq) + (0 if r is None else r * 3)

    def gather_r(self, m, c):
        G = GEO[c]
        at = pl.ds(self.place(c, self.at[G.p], self.at[G.q], self.at[G.r]), 3)
        dst = self.out.at[m, at]
        for d in range(1, G.nr):
            self.send(self.fin.at[m, c], dst, self.s_ag.at[m, c], self.s_gr.at[m, c], G.r, d)
        pltpu.make_async_copy(self.fin.at[m, c], dst, self.s_loc.at[m, c]).start()

    def gather_q(self, m, c):
        G = GEO[c]
        self.wait(self.out.at[m], 3, self.s_loc.at[m, c])
        self.wait(self.out.at[m], 3 * (G.nr - 1), self.s_gr.at[m, c])
        ref = self.out.at[m, pl.ds(self.place(c, self.at[G.p], self.at[G.q]), G.Cq)]
        for d in range(1, G.nq):
            self.send(ref, ref, self.s_ag.at[m, c], self.s_gq.at[m, c], G.q, d)

    def gather_p(self, m, c, s):
        G = GEO[c]
        if s == 1:
            self.wait(self.out.at[m], (G.nq - 1) * G.Cq, self.s_gq.at[m, c])
        else:
            self.wait(self.out.at[m], G.C, self.s_gl.at[m, c, s - 2])
            self.wait(self.out.at[m], G.C, self.s_gright.at[m, c, s - 2])
        n = G.C if s < G.h else G.H
        a = self.out.at[m, pl.ds(self.place(c, self.shift(G.p, 1 - s)), n)]
        b = self.out.at[m, pl.ds(self.place(c, self.shift(G.p, s - 1)) + (G.C - n), n)]
        self.send(a, a, self.s_ag.at[m, c], self.s_gl.at[m, c, s - 1], G.p, 1)
        self.send(b, b, self.s_ag.at[m, c], self.s_gright.at[m, c, s - 1], G.p, -1)

    def gathered(self, m, c):
        G = GEO[c]
        self.wait(self.out.at[m], G.H, self.s_gl.at[m, c, G.h - 1])
        self.wait(self.out.at[m], G.H, self.s_gright.at[m, c, G.h - 1])
        n = 3 * (G.nr - 1) + (G.nq - 1) * G.Cq + 2 * G.C * (G.h - 1) + 2 * G.H
        self.wait(self.g.at[m], n, self.s_ag.at[m, c])


def comm_scratch(k):
    dma = pltpu.SemaphoreType.DMA
    return [
        pltpu.VMEM((k, 3, RECV) + TILE, BF16),
        pltpu.VMEM((RING, 3, OWN) + TILE, BF16),
        pltpu.VMEM((RING, 3, 24) + TILE, F32),
        pltpu.VMEM((RING, 3, 3) + TILE, F32),
        pltpu.VMEM((k, 3, 3) + TILE, BF16),
    ], [dma((k, 3)), dma((k, 3)), dma((k, 3)), dma((k, 3)), dma((k, 3)), dma((k, 3, 3)), dma((k, 3, 3)), dma((k, 3)), dma((k, 3)), dma((k, 3)),
        dma((k, 3)), dma((k, 3)), dma((k, 3, 4)), dma((k, 3, 4))]


def norm_exchange(comm, acc, slots, s_send, s_recv):
    first, total = 0, acc[...]
    for i, ax in enumerate("xyz"):
        n = SIZE[ax]
        slots[pl.ds(first + comm.at[ax], 1)] = total[None]
        ref = slots.at[pl.ds(first + comm.at[ax], 1)]
        for d in range(1, n):
            comm.send(ref, ref, s_send.at[i], s_recv.at[i], ax, d)
        yield
        comm.wait(slots, n - 1, s_recv.at[i])
        total = slots[first]
        for k in range(1, n):
            total = total + slots[first + k]
        first += n
    yield total
    for i, ax in enumerate("xyz"):
        comm.wait(slots, SIZE[ax] - 1, s_send.at[i])


STEPS = FF // 512


def schedule(k):
    ev = []
    for m in range(k):
        for c in range(3):
            for name, t in event_times(m, c, GEO[c].h):
                ev.append((t, len(ev), m, c, name))
    last = max(e[0] for e in ev if e[4] == "third")
    for i, t in enumerate((0.2, 5, 10, 16)):
        ev.append((last + t, len(ev), k, 0, f"norm{i}"))
    ev.sort()
    order = [(e[2], e[3], e[4]) for e in ev]
    for m in range(k):
        for c in range(3):
            names = [e[2] for e in order if e[:2] == (m, c)]
            assert names == [name for name, _ in event_times(m, c, GEO[c].h)], names
    for m in range(k - RING):
        for c in range(3):
            assert order.index((m, c, "first")) < order.index((m + RING, c, "raw"))
            assert order.index((m, c, "third")) < order.index((m + RING, c, "first"))
    return [(t / STEP, m, c, name) for t, _, m, c, name in ev]


def event_times(m, c, h):
    b = STEP * 5 * (m + 1) + PACE * m
    yield "raw", STEP * (5 * m + 4 - 0.5 if c == 0 else 5 * m + 5 - 0.01)
    if c < 2:
        yield "step2", b + RS * 12
    else:
        for s in range(2, h + 1):
            yield f"step{s}", b + RS * (8 + 4 * (s - 2))
    yield "first", b + RS * 20
    yield "second", b + RS * 26
    yield "third", b + RS * 31
    b += RS * 31 + AGX
    yield "gather1", b + 0.1
    yield "gather2", b + AG * 5
    for s in range(1, h + 1):
        yield f"along{s}", b + AG * (11 + (s - 1) * 20 / h)
    yield "end", 10000


STEP = 2.4
PACE = 0
RS = 1
AG = 1
AGX = 0


def gradients_kernel(k, pairs, *refs):
    nl = len(set(pairs))
    lefts, rights = refs[:6], refs[6:12]
    g, out, ss_out, recv, own, own1, own2, fin, acc, slots, lbuf, rbuf, obuf, zero = refs[12:26]
    sems = refs[26:]
    comm = Comm(g, out, recv, own, own1, own2, fin, sems[:14])
    s_send, s_recv, s_left, s_right, s_out, s_zero = sems[14:]
    comm.barrier()
    acc[...] = jnp.zeros_like(acc)
    zero[...] = jnp.zeros_like(zero)

    def left(m):
        return pltpu.make_async_copy(lefts[m], lbuf.at[m % 2], s_left.at[m % 2])

    def right(m, j):
        slot = (m * STEPS + j) % 2
        return pltpu.make_async_copy(rights[m].at[:, pl.ds(j * 512, 512)], rbuf.at[slot], s_right.at[slot])

    def put(m, j):
        slot = (m * STEPS + j) % 2
        return pltpu.make_async_copy(obuf.at[slot], g.at[m, pl.ds(j * 224, 224)], s_out.at[slot])

    def blank(m):
        return pltpu.make_async_copy(zero, g.at[m, pl.ds(1120, 32)], s_zero.at[m])

    left(0).start()
    right(0, 0).start()
    for m in range(k):
        blank(m).start()
    for m in range(k):
        blank(m).wait()

    def last(e):
        return e[3] == "raw" and e[2] > 0

    norm = norm_exchange(comm, acc, slots, s_send, s_recv)

    def run(m, c, name):
        if name.startswith("norm"):
            total = next(norm)
            if name == "norm3":
                ss_out[...] = total
                for _ in norm:
                    pass
        elif name == "raw":
            comm.raw(m, c)
            comm.load(m, c)
        elif name.startswith("step"):
            comm.step(m, c, int(name[4:]))
        elif name == "third":
            acc[...] += comm.third(m, c)
        elif name == "gather1":
            comm.gather_r(m, c)
        elif name == "gather2":
            comm.gather_q(m, c)
        elif name.startswith("along"):
            comm.gather_p(m, c, int(name[5:]))
        elif name == "end":
            comm.rs_sent(m, c)
            comm.gathered(m, c)
        else:
            getattr(comm, name)(m, c)

    events = schedule(k)
    for m in range(k):
        left(m).wait()

        @pl.loop(0, STEPS)
        def _(j):
            right(m, j).wait()

            @pl.when(j < STEPS - 1)
            def _():
                right(m, j + 1).start()

            if m + 1 < k:
                @pl.when(j == STEPS - 1)
                def _():
                    right(m + 1, 0).start()

                @pl.when(j == 1)
                def _():
                    left(m + 1).start()

            @pl.when(j >= 2)
            def _():
                put(m, j - 2).wait()

            slot = (m * STEPS + j) % 2
            v = dot(lbuf[m % 2], rbuf[slot], TN).astype(BF16)
            for c in range(4):
                obuf[slot, c * 56:(c + 1) * 56] = v[:, c * 128:(c + 1) * 128].reshape((56,) + TILE)
            put(m, j).start()
            for n in range(STEPS):
                now = [e[1:] for e in events if int(e[0]) == STEPS * m + n and not last(e)]
                if now:
                    @pl.when(j == n)
                    def _():
                        for e in now:
                            run(*e)

        put(m, STEPS - 2).wait()
        put(m, STEPS - 1).wait()
        for e in events:
            if int(e[0]) == STEPS * m + STEPS - 1 and last(e):
                run(*e[1:])
    for e in events:
        if e[0] >= STEPS * k:
            run(*e[1:])


def gradients(x, dy, w_gate, w_up, w_down):
    a0, z0, dg0, du0, a1, z1, dg1, du1, dh = activations(x, dy, w_gate, w_up, w_down, CH=256)
    return (dy, a1, a1, dh, a0, a0), (z1, dg1, du1, z0, dg0, du0)


def summed(lefts, rights):
    k = 6
    bufs, sems = comm_scratch(k)
    dma = pltpu.SemaphoreType.DMA
    return pl.pallas_call(
        functools.partial(gradients_kernel, k, tuple(range(6))),
        name="gradients",
        out_shape=(jax.ShapeDtypeStruct((k, NT) + TILE, BF16), jax.ShapeDtypeStruct((k, NT) + TILE, BF16), jax.ShapeDtypeStruct((8, 128), F32)),
        in_specs=[ANY] * 12,
        out_specs=(ANY, ANY, pl.BlockSpec(memory_space=pltpu.VMEM)),
        scratch_shapes=bufs + [pltpu.VMEM((8, 128), F32), pltpu.VMEM((16, 8, 128), F32),
                               pltpu.VMEM((2, S, D), BF16), pltpu.VMEM((2, S, 512), BF16), pltpu.VMEM((2, 224) + TILE, BF16), pltpu.VMEM((32,) + TILE, BF16)]
        + sems + [dma((3,)), dma((3,)), dma((2,)), dma((2,)), dma((2,)), dma((k,))],
        cost_estimate=pl.CostEstimate(flops=12 * S * D * FF, bytes_accessed=12 * S * (D + FF), transcendentals=0),
        compiler_params=pltpu.CompilerParams(collective_id=0, has_side_effects=True, vmem_limit_bytes=67043328),
    )(*lefts, *rights)


def solution(mesh):
    def step(x, dy, w_gate, w_up, w_down, m_gate, m_up, m_down, v_gate, v_up, v_down):
        _, g, ss = summed(*gradients(x[0], dy[0], w_gate, w_up, w_down))
        new = [
            adamw(False, 4, ss, g, w_gate, m_gate, v_gate),
            adamw(False, 5, ss, g, w_up, m_up, v_up),
            adamw(True, 3, ss, g, w_down, m_down, v_down),
        ]
        return tuple(one[which] for which in range(3) for one in new)

    return jax.shard_map(
        step,
        mesh=mesh,
        in_specs=(P(("rep", "dp"), None, None),) * 2 + (P(None, None, None),) * 9,
        out_specs=(P("rep", None, None),) * 9,
        check_vma=False,
    )
```

```python
import functools

import jax
import jax.numpy as jnp
from jax import lax
from jax.experimental import pallas as pl
from jax.experimental.pallas import tpu as pltpu
from jax.sharding import PartitionSpec as P

F32, BF16 = jnp.float32, jnp.bfloat16
S, D, FF = 2048, 896, 2560
MESH = pl.DeviceIdType.MESH
ANY = pl.BlockSpec(memory_space=pl.ANY)
TILE = (16, 128)
NT = 1152
SLAB = 384
SQUARES = (8, 128)
ROOM, MOST = 63 * 2**20, 67043328
THREE = range(3)
SHARE = 3
LANES, BANDS = 128, 56
SIZE = {"x": 4, "y": 4, "z": 8}
STRIDE = {"x": 32, "y": 8, "z": 1}
COLORS = ((("x", "y", "z"), ("y", "x", "z"), ("z", "x", "y")), (("x", "y", "z"), ("y", "x", "z"), ("z", "y", "x")))
RECV = 381
NN = (((1,), (0,)), ((), ()))
NT_ = (((1,), (1,)), ((), ()))
TN = (((0,), (0,)), ((), ()))


def dot(a, b, dims=NN):
    return lax.dot_general(a, b, dims, preferred_element_type=F32)


def sigmoid(x):
    return 0.5 + 0.5 * jnp.tanh(0.5 * x)


def norm_of(h):
    wide = h.astype(F32)
    return wide, lax.rsqrt(jnp.mean(wide * wide, -1, keepdims=True) + 1e-6)


def activations_kernel(CH, x_ref, dy_ref, wg_hbm, wu_hbm, wd_hbm, a0_ref, z0_ref, dg0_ref, du0_ref, a1_ref, z1_ref, dg1_ref, du1_ref, dh_ref, wg, wu, wd, gate0, up0, sem):
    first = pl.program_id(0) == 0
    n = FF // CH
    copies = [[pltpu.make_async_copy(hbm.at[layer], vmem.at[layer], sem.at[layer, k]) for k, (hbm, vmem) in enumerate(((wg_hbm, wg), (wu_hbm, wu), (wd_hbm, wd)))] for layer in range(2)]

    @pl.when(first)
    def _():
        for layer in range(2):
            for copy in copies[layer]:
                copy.start()
        copies[0][0].wait()
        copies[0][1].wait()

    x = x_ref[...]
    dy = dy_ref[...]
    wide, scale = norm_of(x)
    a = (wide * scale).astype(BF16)
    a0_ref[...] = a
    for j in range(n):
        at = pl.ds(j * CH, CH)
        gate, up = dot(a, wg[0, :, at]), dot(a, wu[0, :, at])
        gate0[:, at] = gate
        up0[:, at] = up
        z0_ref[:, at] = (gate * sigmoid(gate) * up).astype(BF16)

    @pl.when(first)
    def _():
        copies[0][2].wait()

    h = x + dot(z0_ref[...], wd[0]).astype(BF16)
    wide, scale = norm_of(h)
    a = (wide * scale).astype(BF16)
    a1_ref[...] = a

    @pl.when(first)
    def _():
        for copy in copies[1]:
            copy.wait()

    def back(gate, up, dz, dg_ref, du_ref, at):
        dz = dz.astype(BF16).astype(F32)
        sig = sigmoid(gate)
        silu = gate * sig
        du_ref[:, at] = (dz * silu).astype(BF16)
        dg_ref[:, at] = (dz * up * (sig + silu * (1.0 - sig))).astype(BF16)
        return silu

    for j in range(n):
        at = pl.ds(j * CH, CH)
        gate, up, dz = dot(a, wg[1, :, at]), dot(a, wu[1, :, at]), dot(dy, wd[1, at, :], NT_)
        z1_ref[:, at] = (back(gate, up, dz, dg1_ref, du1_ref, at) * up).astype(BF16)
    da = (dot(dg1_ref[...], wg[1], NT_).astype(BF16) + dot(du1_ref[...], wu[1], NT_).astype(BF16)).astype(F32)
    by_mean = jnp.sum(da * wide, -1, keepdims=True) * (-1.0 / D) * (scale * scale * scale)
    dh = dy + (da * scale + by_mean * wide).astype(BF16)
    dh_ref[...] = dh
    for j in range(n):
        at = pl.ds(j * CH, CH)
        back(gate0[:, at], up0[:, at], dot(dh, wd[0, at, :], NT_), dg0_ref, du0_ref, at)


def activations(x, dy, w_gate, w_up, w_down, T=256, CH=512):
    row = lambda w: pl.BlockSpec((T, w), lambda i: (i, 0))
    widths = (D, FF, FF, FF, D, FF, FF, FF, D)
    return pl.pallas_call(
        functools.partial(activations_kernel, CH),
        name="activations",
        grid=(S // T,),
        in_specs=[row(D), row(D), ANY, ANY, ANY],
        out_specs=[row(w) for w in widths],
        out_shape=[jax.ShapeDtypeStruct((S, w), BF16) for w in widths],
        scratch_shapes=[pltpu.VMEM((2, D, FF), BF16), pltpu.VMEM((2, D, FF), BF16), pltpu.VMEM((2, FF, D), BF16), pltpu.VMEM((T, FF), F32), pltpu.VMEM((T, FF), F32),
                        pltpu.SemaphoreType.DMA((2, 3))],
        cost_estimate=pl.CostEstimate(flops=18 * S * D * FF, bytes_accessed=2 * S * (6 * FF + 5 * D) + 12 * D * FF, transcendentals=2 * S * FF),
        compiler_params=pltpu.CompilerParams(vmem_limit_bytes=ROOM),
    )(x, dy, w_gate, w_up, w_down)


NB = 2


def adamw_kernel(B, ss_ref, g_hbm, *refs):
    ins, outs = [refs[i:9:3] for i in THREE], [refs[9 + i:18:3] for i in THREE]
    gb, wb, mb, vb, wo, mo, vo = [refs[18 + 3 * i:21 + 3 * i] for i in range(7)]
    s_in, s_out = refs[39:]
    n = 20 // B
    total = jnp.sum(ss_ref[...], keepdims=True)
    f = jnp.minimum(1.0, 0.5 * lax.rsqrt(total / (6 * D * FF) + 1e-30))

    def block(ref, k, i):
        at = pl.ds(pl.multiple_of(i % n * (LANES * B), LANES * B), LANES * B)
        return ref.at[i // n, at, :] if k == 2 else ref.at[i // n, :, at]

    def loads(k, i):
        g = g_hbm.at[(4, 5, 3)[k] - 3 * (i // n), pl.ds(i % n * (BANDS * B), BANDS * B)]
        pairs = [(g, gb[k])] + [(block(h, k, i), v[k]) for h, v in zip(ins[k], (wb, mb, vb))]
        return [pltpu.make_async_copy(h, v.at[i % NB], s_in.at[k, i % NB, p]) for p, (h, v) in enumerate(pairs)]

    def stores(k, i):
        return [pltpu.make_async_copy(v[k].at[i % NB], block(h, k, i), s_out.at[k, i % NB, p]) for p, (h, v) in enumerate(zip(outs[k], (wo, mo, vo)))]

    def part(k, slot, g, r, c):
        g = g.astype(F32) * f
        m = 0.9 * mb[k][slot, r, c] + 0.1 * g
        v = 0.95 * vb[k][slot, r, c] + 0.05 * g * g
        w = wb[k][slot, r, c].astype(F32)
        wo[k][slot, r, c] = (w - 0.02 * (m * lax.rsqrt(v + 1e-8) + 0.1 * w)).astype(BF16)
        mo[k][slot, r, c] = m
        vo[k][slot, r, c] = v

    for i in range(NB):
        for k in THREE:
            for copy in loads(k, i):
                copy.start()

    @pl.loop(0, 2 * n)
    def _(i):
        slot = i % NB
        for k in THREE:
            for copy in loads(k, i):
                copy.wait()

            @pl.when(i >= NB)
            def _():
                for copy in stores(k, i - NB):
                    copy.wait()

            if k < 2:
                @pl.loop(0, BANDS)
                def _(r):
                    rows = pl.ds(pl.multiple_of(r * 16, 16), 16)
                    for j in range(B):
                        part(k, slot, gb[k][slot, j * BANDS + r], rows, slice(j * LANES, (j + 1) * LANES))
            else:
                @pl.loop(0, 7)
                def _(r):
                    for j in range(B):
                        g = gb[k][slot, pl.ds(j * BANDS + r * 8, 8)].reshape(LANES, LANES).T
                        part(k, slot, g, slice(j * LANES, (j + 1) * LANES), pl.ds(pl.multiple_of(r * LANES, LANES), LANES))

            for copy in stores(k, i):
                copy.start()

            @pl.when(i + NB < 2 * n)
            def _():
                for copy in loads(k, i + NB):
                    copy.start()

    for i in range(2 * n - NB, 2 * n):
        for k in THREE:
            for copy in stores(k, i):
                copy.wait()


def adamw(ss, g, w, m, v, B=4):
    n = 6 * D * FF
    shapes = ((NB, D, LANES * B), (NB, D, LANES * B), (NB, LANES * B, D))
    three = lambda t: [pltpu.VMEM(s, t) for s in shapes]
    return pl.pallas_call(
        functools.partial(adamw_kernel, B),
        name="adamw",
        in_specs=[pl.BlockSpec(memory_space=pltpu.VMEM)] + [ANY] * 10,
        out_specs=[ANY] * 9,
        out_shape=[jax.ShapeDtypeStruct(a.shape, t) for t in (BF16, F32, F32) for a in w],
        scratch_shapes=[pltpu.VMEM((NB, BANDS * B) + TILE, BF16)] * 3 + three(BF16) + three(F32) * 2 + three(BF16) + three(F32) * 2
        + [pltpu.SemaphoreType.DMA((3, NB, 4)), pltpu.SemaphoreType.DMA((3, NB, 3))],
        cost_estimate=pl.CostEstimate(flops=20 * n, bytes_accessed=22 * n, transcendentals=n),
        compiler_params=pltpu.CompilerParams(vmem_limit_bytes=ROOM),
    )(ss, g, *w, *m, *v)


class Geo:
    def __init__(self, c, axes):
        self.c = c
        self.p, self.q, self.r = axes
        self.n, self.nq, self.nr = (SIZE[a] for a in axes)
        self.h = self.n // 2
        self.C = SLAB // self.n
        self.H = self.C // 2
        self.Cq = self.C // self.nq
        assert self.Cq == 3 * self.nr
        self.long = self.nr == 8
        self.own = 2 * self.H + 2 * self.C * (self.h - 2) + self.C
        self.p2 = 2 * self.H + 2 * self.C * (self.h - 1)
        self.p3 = self.p2 + (self.nq - 1) * self.Cq
        assert self.p3 + 3 * (self.nr - 1) == RECV

    def L(self, s):
        return 2 * self.H + (s - 2) * 2 * self.C

    def R(self, s):
        return self.L(s) + self.C

    def own_step(self, s):
        return 2 * self.H + (s - 3) * 2 * self.C

    @property
    def own_mine(self):
        return 2 * self.H + 2 * self.C * (self.h - 2)


GEO = [[Geo(c, axes) for c, axes in enumerate(colors)] for colors in COLORS]


def geo(m, c):
    return GEO[m % 2][c]


OWN = max(g.own for g in GEO[0])
RING = 4


def add_loop(n, body, unroll):
    assert n % unroll == 0
    if n == unroll:
        body(0, unroll)
    else:
        pl.loop(0, n // unroll)(lambda i: body(i * unroll, unroll))


class Comm:
    def __init__(self, g, out, recv, own, own1, own2, fin, sems):
        self.g, self.out, self.recv, self.own, self.own1, self.own2, self.fin = g, out, recv, own, own1, own2, fin
        (self.s_rs, self.s_ag, self.s_own, self.s_a, self.s_b, self.s_l, self.s_r, self.s_p2, self.s_p3, self.s_loc,
         self.s_gr, self.s_gq, self.s_gl, self.s_gright, self.s_za, self.s_zg, self.s_qa, self.s_gh) = sems
        me = lax.axis_index("dp")
        self.me = me
        self.at = {"x": me // 32, "y": me // 8 % 4, "z": me % 8}
        self.even = lax.rem(me, 2) == 0
        self.way = 1 - 2 * lax.rem(me, 2)

    def shift(self, ax, d):
        return lax.rem(self.at[ax] + (d + SIZE[ax]), SIZE[ax])

    def peer(self, ax, d):
        return {"dp": self.me + (self.shift(ax, d) - self.at[ax]) * STRIDE[ax]}

    def barrier(self):
        b = pltpu.get_barrier_semaphore()
        count = 0
        for ax in "xyz":
            for d in range(1, SIZE[ax]):
                pl.semaphore_signal(b, inc=1, device_id=self.peer(ax, d), device_id_type=MESH)
                count += 1
        pl.semaphore_wait(b, count)

    def send(self, src, dst, ssem, rsem, ax, d):
        pltpu.make_async_remote_copy(src_ref=src, dst_ref=dst, send_sem=ssem, recv_sem=rsem, device_id=self.peer(ax, d), device_id_type=MESH).start()

    def wait(self, ref, n, sem):
        pltpu.make_async_copy(ref.at[pl.ds(0, n)], ref.at[pl.ds(0, n)], sem).wait()

    def got(self, m, c, n, sem):
        self.wait(self.recv.at[m, c], n, sem)

    def raw(self, m, c):
        G = geo(m, c)
        g, rv = self.g.at[m], self.recv.at[m, c]
        chunk = lambda d: c * SLAB + self.shift(G.p, d) * G.C
        ss = self.s_rs.at[m, c]
        self.send(g.at[pl.ds(chunk(G.h), G.H)], rv.at[pl.ds(0, G.H)], ss, self.s_a.at[m, c], G.p, 1)
        self.send(g.at[pl.ds(chunk(G.h) + G.H, G.H)], rv.at[pl.ds(G.H, G.H)], ss, self.s_b.at[m, c], G.p, -1)
        self.send(g.at[pl.ds(chunk(G.h - 1) + G.H, G.H)], rv.at[pl.ds(G.L(2) + G.H, G.H)], ss, self.s_l.at[m, c, 0], G.p, 1)
        self.send(g.at[pl.ds(chunk(1 - G.h), G.H)], rv.at[pl.ds(G.R(2), G.H)], ss, self.s_r.at[m, c, 0], G.p, -1)

    def load(self, m, c):
        G = geo(m, c)
        g, own = self.g.at[m], self.own.at[m % RING, c]
        chunk = lambda d: c * SLAB + self.shift(G.p, d) * G.C
        parts = [(chunk(G.h - 1), 0, G.H), (chunk(1 - G.h) + G.H, G.H, G.H)]
        for s in range(3, G.h + 1):
            parts += [(chunk(G.h - s + 1), G.own_step(s), G.C), (chunk(s - G.h - 1), G.own_step(s) + G.C, G.C)]
        parts += [(chunk(0), G.own_mine, G.C)]
        for src, dst, n in parts:
            pltpu.make_async_copy(g.at[pl.ds(src, n)], own.at[pl.ds(dst, n)], self.s_own.at[m, c]).start()

    def add_in(self, m, c, at, own_at, n):
        rv, own = self.recv.at[m, c], self.own.at[m % RING, c]

        def body(i, k):
            rv[pl.ds(at + i, k)] = (rv[pl.ds(at + i, k)].astype(F32) + own[pl.ds(own_at + i, k)].astype(F32)).astype(BF16)

        add_loop(n, body, 8)

    def step(self, m, c, s):
        G = geo(m, c)
        rv = self.recv.at[m, c]
        ss = self.s_rs.at[m, c]
        if s == 2:
            self.wait(self.own.at[m % RING, c], G.own, self.s_own.at[m, c])
            self.got(m, c, G.H, self.s_a.at[m, c])
            self.add_in(m, c, 0, 0, G.H)
            self.got(m, c, G.H, self.s_b.at[m, c])
            self.send(rv.at[pl.ds(0, G.H)], rv.at[pl.ds(G.L(2), G.H)], ss, self.s_l.at[m, c, 0], G.p, 1)
            self.add_in(m, c, G.H, G.H, G.H)
            self.send(rv.at[pl.ds(G.H, G.H)], rv.at[pl.ds(G.R(2) + G.H, G.H)], ss, self.s_r.at[m, c, 0], G.p, -1)
        else:
            self.got(m, c, G.C, self.s_l.at[m, c, s - 3])
            self.add_in(m, c, G.L(s - 1), G.own_step(s), G.C)
            self.got(m, c, G.C, self.s_r.at[m, c, s - 3])
            self.send(rv.at[pl.ds(G.L(s - 1), G.C)], rv.at[pl.ds(G.L(s), G.C)], ss, self.s_l.at[m, c, s - 2], G.p, 1)
            self.add_in(m, c, G.R(s - 1), G.own_step(s) + G.C, G.C)
            self.send(rv.at[pl.ds(G.R(s - 1), G.C)], rv.at[pl.ds(G.R(s), G.C)], ss, self.s_r.at[m, c, s - 2], G.p, -1)

    def first(self, m, c):
        G = geo(m, c)
        rv, own = self.recv.at[m, c], self.own.at[m % RING, c]
        l, r, mine = G.L(G.h), G.R(G.h), G.own_mine
        self.got(m, c, G.C, self.s_l.at[m, c, G.h - 2])
        self.got(m, c, G.C, self.s_r.at[m, c, G.h - 2])

        def total(i, k):
            return own[pl.ds(mine + i, k)].astype(F32) + rv[pl.ds(l + i, k)].astype(F32) + rv[pl.ds(r + i, k)].astype(F32)

        half = G.Cq // 2

        def keep(at, start, n):
            def body(i, k):
                self.own1[m % 2, c, pl.ds(at + i, k)] = total(start + i, k)

            add_loop(n, body, 2)

        def body(i, k):
            rv[pl.ds(l + i, k)] = total(i, k).astype(BF16)

        chunk = lambda d: self.shift(G.q, d) * G.Cq
        keep(0, chunk(0), G.Cq)
        keep(G.Cq, chunk(1), half)
        keep(G.Cq + half, chunk(-1) + half, half)
        add_loop(G.C, body, 8)

        def part(start, to, at, sem):
            self.send(rv.at[pl.ds(l + start, half)], rv.at[pl.ds(G.p2 + at, half)], self.s_rs.at[m, c], sem.at[m, c], G.q, to)

        part(chunk(2), 1, 0, self.s_qa)
        part(chunk(2) + half, -1, half, self.s_qa)
        part(chunk(1) + half, 1, G.Cq + half, self.s_p2)
        part(chunk(-1), -1, 2 * G.Cq, self.s_p2)

    def mid(self, m, c):
        G = geo(m, c)
        rv, half = self.recv.at[m, c], G.Cq // 2
        self.got(m, c, G.Cq, self.s_qa.at[m, c])

        def body(i, k):
            at = pl.ds(G.p2 + i, k)
            rv[at] = (self.own1[m % 2, c, pl.ds(G.Cq + i, k)] + rv[at].astype(F32)).astype(BF16)

        add_loop(G.Cq, body, 4)
        for at, dst, to in ((0, G.Cq, 1), (half, 2 * G.Cq + half, -1)):
            self.send(rv.at[pl.ds(G.p2 + at, half)], rv.at[pl.ds(G.p2 + dst, half)], self.s_rs.at[m, c], self.s_p2.at[m, c], G.q, to)

    def second(self, m, c):
        G = geo(m, c)
        rv = self.recv.at[m, c]
        left, right = G.p2 + G.Cq, G.p2 + 2 * G.Cq
        self.got(m, c, 2 * G.Cq, self.s_p2.at[m, c])

        def total(i, k):
            return self.own1[m % 2, c, pl.ds(i, k)] + rv[pl.ds(left + i, k)].astype(F32) + rv[pl.ds(right + i, k)].astype(F32)

        for k, d in enumerate((0, 2, -2) if G.long else (0,)):
            self.own2[m % RING, c, k] = total(self.shift(G.r, d) * SHARE, SHARE)

        def body(i, k):
            rv[pl.ds(left + i, k)] = total(i, k).astype(BF16)

        add_loop(G.Cq, body, 4)

        def piece(by, to, slot, sem):
            self.send(rv.at[pl.ds(left + self.shift(G.r, by) * SHARE, SHARE)], rv.at[pl.ds(G.p3 + SHARE * slot, SHARE)], self.s_rs.at[m, c], sem.at[m, c], G.r, to)

        if G.long:
            piece(3, 1, 0, self.s_za)
            piece(-3, -1, 1, self.s_za)
            piece(4, 2 * self.way, 2, self.s_za)
            piece(1, 1, 3, self.s_p3)
            piece(-1, -1, 4, self.s_p3)
        else:
            for d in range(1, G.nr):
                piece(d, d, d - 1, self.s_p3)

    def zmid(self, m, c):
        G = geo(m, c)
        rv = self.recv.at[m, c]
        self.got(m, c, 3 * SHARE, self.s_za.at[m, c])
        came = [rv[pl.ds(G.p3 + SHARE * i, SHARE)].astype(F32) for i in range(3)]
        ahead = self.own2[m % RING, c, 1] + came[0] + jnp.where(self.even, came[2], 0.0)
        behind = self.own2[m % RING, c, 2] + came[1] + jnp.where(self.even, 0.0, came[2])
        for slot, (way, piece) in enumerate(((2, ahead), (-2, behind))):
            rv[pl.ds(G.p3 + SHARE * slot, SHARE)] = piece.astype(BF16)
        for slot, way in enumerate((2, -2)):
            self.send(rv.at[pl.ds(G.p3 + SHARE * slot, SHARE)], rv.at[pl.ds(G.p3 + SHARE * (5 + slot), SHARE)], self.s_rs.at[m, c], self.s_p3.at[m, c], G.r, way)

    def third(self, m, c):
        G = geo(m, c)
        rv = self.recv.at[m, c]
        first, n = (3, 4) if G.long else (0, 3)
        self.got(m, c, SHARE * n, self.s_p3.at[m, c])
        t = self.own2[m % RING, c, 0]
        for i in range(first, first + n):
            t = t + rv[pl.ds(G.p3 + SHARE * i, SHARE)].astype(F32)
        t = t.astype(BF16)
        self.fin[m, c] = t
        t = t.astype(F32)
        return jnp.sum((t * t).reshape(6, 8, 128), axis=0)

    def rs_sent(self, m, c):
        G = geo(m, c)
        n = 4 * G.H + 2 * G.H + 2 * G.C * (G.h - 2) + (G.nq - 1) * G.Cq + (G.nr - 1) * 3
        self.wait(self.g.at[m], n, self.s_rs.at[m, c])

    def place(self, m, c, p, q=None, r=None):
        G = geo(m, c)
        return c * SLAB + p * G.C + (0 if q is None else q * G.Cq) + (0 if r is None else r * SHARE)

    def gather_r(self, m, c):
        G = geo(m, c)
        dst = self.out.at[m, pl.ds(self.place(m, c, self.at[G.p], self.at[G.q], self.at[G.r]), SHARE)]
        for d in (1, -1, 2, -2) if G.long else range(1, G.nr):
            self.send(self.fin.at[m, c], dst, self.s_ag.at[m, c], (self.s_zg if G.long else self.s_gr).at[m, c], G.r, d)
        pltpu.make_async_copy(self.fin.at[m, c], dst, self.s_loc.at[m, c]).start()

    def zpass(self, m, c):
        G = geo(m, c)
        self.wait(self.out.at[m], 4 * SHARE, self.s_zg.at[m, c])
        for by, to in ((-2, 1), (2, -1), (-2 * self.way, 2 * self.way)):
            ref = self.out.at[m, pl.ds(self.place(m, c, self.at[G.p], self.at[G.q], self.shift(G.r, by)), SHARE)]
            self.send(ref, ref, self.s_ag.at[m, c], self.s_gr.at[m, c], G.r, to)

    def gather_q(self, m, c):
        G = geo(m, c)
        self.wait(self.out.at[m], SHARE, self.s_loc.at[m, c])
        self.wait(self.out.at[m], 3 * SHARE, self.s_gr.at[m, c])
        ref = self.out.at[m, pl.ds(self.place(m, c, self.at[G.p], self.at[G.q]), G.Cq)]
        for d in (1, -1):
            self.send(ref, ref, self.s_ag.at[m, c], self.s_gq.at[m, c], G.q, d)

    def qpass(self, m, c):
        G = geo(m, c)
        self.wait(self.out.at[m], 2 * G.Cq, self.s_gq.at[m, c])
        half = G.Cq // 2
        for d, more in ((1, 0), (-1, half)):
            ref = self.out.at[m, pl.ds(self.place(m, c, self.at[G.p], self.shift(G.q, -d)) + more, half)]
            self.send(ref, ref, self.s_ag.at[m, c], self.s_gh.at[m, c], G.q, d)

    def gather_p(self, m, c, s):
        G = geo(m, c)
        if s == 1:
            self.wait(self.out.at[m], G.Cq, self.s_gh.at[m, c])
        else:
            self.wait(self.out.at[m], G.C, self.s_gl.at[m, c, s - 2])
            self.wait(self.out.at[m], G.C, self.s_gright.at[m, c, s - 2])
        n = G.C if s < G.h else G.H
        a = self.out.at[m, pl.ds(self.place(m, c, self.shift(G.p, 1 - s)), n)]
        b = self.out.at[m, pl.ds(self.place(m, c, self.shift(G.p, s - 1)) + (G.C - n), n)]
        self.send(a, a, self.s_ag.at[m, c], self.s_gl.at[m, c, s - 1], G.p, 1)
        self.send(b, b, self.s_ag.at[m, c], self.s_gright.at[m, c, s - 1], G.p, -1)

    def gathered(self, m, c):
        G = geo(m, c)
        self.wait(self.out.at[m], G.H, self.s_gl.at[m, c, G.h - 1])
        self.wait(self.out.at[m], G.H, self.s_gright.at[m, c, G.h - 1])
        n = 3 * (G.nr - 1) + (G.nq - 1) * G.Cq + 2 * G.C * (G.h - 1) + 2 * G.H
        self.wait(self.g.at[m], n, self.s_ag.at[m, c])


def comm_scratch(k):
    dma = pltpu.SemaphoreType.DMA
    one = dma((k, 3))
    return [
        pltpu.VMEM((k, 3, RECV) + TILE, BF16),
        pltpu.VMEM((RING, 3, OWN) + TILE, BF16),
        pltpu.VMEM((2, 3, 48) + TILE, F32),
        pltpu.VMEM((RING, 3, 3, SHARE) + TILE, F32),
        pltpu.VMEM((k, 3, 3) + TILE, BF16),
    ], [one] * 5 + [dma((k, 3, 3))] * 2 + [one] * 5 + [dma((k, 3, 4))] * 2 + [one] * 4


def norm_exchange(comm, acc, slots, s_send, s_recv):
    first, total = 0, acc[...]
    for i, ax in enumerate("xyz"):
        n = SIZE[ax]
        slots[pl.ds(first + comm.at[ax], 1)] = total[None]
        ref = slots.at[pl.ds(first + comm.at[ax], 1)]
        for d in range(1, n):
            comm.send(ref, ref, s_send.at[i], s_recv.at[i], ax, d)
        yield
        comm.wait(slots, n - 1, s_recv.at[i])
        total = slots[first]
        for k in range(1, n):
            total = total + slots[first + k]
        first += n
    yield total
    for i, ax in enumerate("xyz"):
        comm.wait(slots, SIZE[ax] - 1, s_send.at[i])


WIDE = 512
STEPS = FF // WIDE


LINK, PRODUCT, NEAR, FAR, HOP = 0.092, 2.6, 2.0, 3.1, 0.7
STORED, BRIEF, ADDS, ADD = 2.5, 0.05, 0.1, 0.002


def tasks(G):
    def each(ax, tiles, late, name):
        return [(ax, (tiles, 0), late, name), (ax, (0, tiles), late, name)]

    follow = lambda s: "first" if s == G.h else f"step{s + 1}"
    out = [("raw", (), each(G.p, G.H, FAR, "step2") + each(G.p, G.H, FAR, follow(2)), BRIEF)]
    for s in range(2, G.h + 1):
        n = G.H if s == 2 else G.C
        out.append((f"step{s}", (f"step{s}",), each(G.p, n, NEAR, follow(s)), ADDS + 4 * ADD * n))
    half = G.Cq / 2
    out.append(("first", ("first",), each(G.q, half, NEAR, "mid") + each(G.q, half, NEAR, "second"), ADDS + 3 * ADD * (G.C + G.Cq)))
    out.append(("mid", ("mid",), each(G.q, half, NEAR, "second"), ADDS + 2 * ADD * G.Cq))
    if G.long:
        far = each(G.r, SHARE, NEAR, "zmid") + [(G.r, (SHARE, SHARE), NEAR + HOP, "zmid")]
        out.append(("second", ("second",), far + each(G.r, SHARE, NEAR, "third"), ADDS + 4 * ADD * G.Cq))
        out.append(("zmid", ("zmid",), each(G.r, 2 * SHARE, NEAR + HOP, "third"), ADDS))
        out.append(("third", ("third",), [], ADDS + BRIEF))
        out.append(("gather1", (), each(G.r, SHARE, STORED, "zpass") + each(G.r, 2 * SHARE, STORED + HOP, "zpass"), BRIEF))
        out.append(("zpass", ("zpass",), each(G.r, SHARE, FAR, "gather2") + [(G.r, (SHARE, SHARE), FAR + HOP, "gather2")], BRIEF))
    else:
        out.append(("second", ("second",), each(G.r, SHARE, NEAR, "third") + [(G.r, (SHARE, SHARE), NEAR + HOP, "third")], ADDS + 4 * ADD * G.Cq))
        out.append(("third", ("third",), [], ADDS + BRIEF))
        out.append(("gather1", (), each(G.r, SHARE, STORED, "gather2") + [(G.r, (SHARE, SHARE), STORED + HOP, "gather2")], BRIEF))
    out.append(("gather2", ("gather2",), each(G.q, G.Cq, FAR, "qpass"), BRIEF))
    out.append(("qpass", ("qpass",), each(G.q, half, FAR, "along1"), BRIEF))
    for s in range(1, G.h + 1):
        out.append((f"along{s}", (f"along{s}",), each(G.p, G.C if s < G.h else G.H, FAR, f"along{s + 1}"), BRIEF))
    out.append(("end", (f"along{G.h + 1}",), [], BRIEF))
    return out


def schedule(k):
    lists = {(m, c): tasks(geo(m, c)) for m in range(k) for c in THREE}
    place = dict.fromkeys(lists, 0)
    arrived, free, done, order = {}, {}, set(), []
    now, steps = 3.0, 0
    while any(place[mc] < len(lists[mc]) for mc in lists):
        ready = []
        for (m, c), tasks_ in lists.items():
            if place[m, c] == len(tasks_):
                continue
            name, waits, _, _ = tasks_[place[m, c]]
            if name == "raw" and (steps < STEPS * m + (3 if c == 0 else STEPS) or m >= RING and (m - RING, c, "first") not in done):
                continue
            if name == "first" and (m >= RING and (m - RING, c, "third") not in done or m >= 2 and (m - 2, c, "second") not in done):
                continue
            when = max((arrived[m, c, w] for w in waits), default=0.0)
            ready.append((when, (name != "raw", m, c), m, c))
        here = [r for r in ready if r[0] <= now]
        if not here and steps < STEPS * k:
            now, steps = now + PRODUCT, steps + 1
            continue
        when, _, m, c = min(here, key=lambda r: r[1]) if here else min(ready)
        name, _, sends, takes = lists[m, c][place[m, c]]
        now = max(now, when) + takes
        for ax, tiles, late, to in sends:
            end = now
            for way in range(2):
                if tiles[way]:
                    end = free[ax, way] = max(free.get((ax, way), 0.0), now) + LINK * tiles[way]
            arrived[m, c, to] = max(arrived.get((m, c, to), 0.0), end + late)
        place[m, c] += 1
        done.add((m, c, name))
        order.append((steps, m, c, name))
    order = [e for e in order if e[3] != "end"]
    last = max(i for i, e in enumerate(order) if e[3] == "third")
    for i in range(4):
        after = min(last + 1 + NORM_GAP * i, len(order))
        order.insert(after, (order[after - 1][0], k, 0, f"norm{i}"))
    return order


NORM_GAP = 12


def gradients_kernel(k, pairs, *refs):
    lefts, rights = refs[:6], refs[6:12]
    g, out, ss_out, recv, own, own1, own2, fin, acc, slots, lbuf, rbuf, obuf, zero = refs[12:26]
    sems = refs[26:]
    comm = Comm(g, out, recv, own, own1, own2, fin, sems[:18])
    s_send, s_recv, s_left, s_right, s_out, s_zero = sems[18:]
    comm.barrier()
    acc[...] = jnp.zeros_like(acc)
    zero[...] = jnp.zeros_like(zero)

    def left(m):
        return pltpu.make_async_copy(lefts[m], lbuf.at[m % 2], s_left.at[m % 2])

    def right(m, j):
        slot = (m * STEPS + j) % 2
        return pltpu.make_async_copy(rights[m].at[:, pl.ds(j * WIDE, WIDE)], rbuf.at[slot], s_right.at[slot])

    def put(m, j):
        slot = (m * STEPS + j) % 2
        return pltpu.make_async_copy(obuf.at[slot], g.at[m, pl.ds(j * 4 * BANDS, 4 * BANDS)], s_out.at[slot])

    def blank(m):
        return pltpu.make_async_copy(zero, g.at[m, pl.ds(1120, 32)], s_zero.at[m])

    left(0).start()
    right(0, 0).start()
    for m in range(k):
        blank(m).start()
    for m in range(k):
        blank(m).wait()

    norm = norm_exchange(comm, acc, slots, s_send, s_recv)

    def run(m, c, name):
        if name.startswith("norm"):
            total = next(norm)
            if name == "norm3":
                ss_out[...] = total
                for _ in norm:
                    pass
        elif name == "raw":
            comm.raw(m, c)
            comm.load(m, c)
        elif name.startswith("step"):
            comm.step(m, c, int(name[4:]))
        elif name == "third":
            acc[...] += comm.third(m, c)
        elif name == "gather1":
            comm.gather_r(m, c)
        elif name == "gather2":
            comm.gather_q(m, c)
        elif name.startswith("along"):
            comm.gather_p(m, c, int(name[5:]))
        else:
            getattr(comm, name)(m, c)

    events = schedule(k)
    for m in range(k):
        left(m).wait()

        @pl.loop(0, STEPS)
        def _(j):
            right(m, j).wait()

            @pl.when(j < STEPS - 1)
            def _():
                right(m, j + 1).start()

            if m + 1 < k:
                @pl.when(j == STEPS - 1)
                def _():
                    right(m + 1, 0).start()

                @pl.when(j == 1)
                def _():
                    left(m + 1).start()

            slot = (m * STEPS + j) % 2
            v = dot(lbuf[m % 2], rbuf[slot], TN).astype(BF16)
            for c in range(WIDE // LANES):
                obuf[slot, c * BANDS:(c + 1) * BANDS] = v[:, c * LANES:(c + 1) * LANES].reshape((BANDS,) + TILE)
            put(m, j).start()

            @pl.when(j >= 1)
            def _():
                put(m, j - 1).wait()

            for n in range(STEPS - 1):
                now = [e[1:] for e in events if e[0] == STEPS * m + n + 1]
                if now:
                    @pl.when(j == n)
                    def _():
                        for e in now:
                            run(*e)

        put(m, STEPS - 1).wait()
        for e in events:
            if e[0] == STEPS * (m + 1):
                run(*e[1:])
    for m in range(k):
        for c in THREE:
            comm.rs_sent(m, c)
            comm.gathered(m, c)


def gradients(x, dy, w_gate, w_up, w_down):
    a0, z0, dg0, du0, a1, z1, dg1, du1, dh = activations(x, dy, w_gate, w_up, w_down, CH=256)
    return (dy, a1, a1, dh, a0, a0), (z1, dg1, du1, z0, dg0, du0)


def summed(lefts, rights):
    k = 6
    bufs, sems = comm_scratch(k)
    dma = pltpu.SemaphoreType.DMA
    return pl.pallas_call(
        functools.partial(gradients_kernel, k, tuple(range(6))),
        name="gradients",
        out_shape=(jax.ShapeDtypeStruct((k, NT) + TILE, BF16), jax.ShapeDtypeStruct((k, NT) + TILE, BF16), jax.ShapeDtypeStruct(SQUARES, F32)),
        in_specs=[ANY] * 12,
        out_specs=(ANY, ANY, pl.BlockSpec(memory_space=pltpu.VMEM)),
        scratch_shapes=bufs + [pltpu.VMEM(SQUARES, F32), pltpu.VMEM((16,) + SQUARES, F32),
                               pltpu.VMEM((2, S, D), BF16), pltpu.VMEM((2, S, 512), BF16), pltpu.VMEM((2, 224) + TILE, BF16), pltpu.VMEM((32,) + TILE, BF16)]
        + sems + [dma((3,))] * 2 + [dma((2,))] * 3 + [dma((k,))],
        cost_estimate=pl.CostEstimate(flops=12 * S * D * FF, bytes_accessed=12 * S * (D + FF), transcendentals=0),
        compiler_params=pltpu.CompilerParams(collective_id=0, has_side_effects=True, vmem_limit_bytes=MOST),
    )(*lefts, *rights)


def solution(mesh):
    def step(x, dy, w_gate, w_up, w_down, m_gate, m_up, m_down, v_gate, v_up, v_down):
        _, g, ss = summed(*gradients(x[0], dy[0], w_gate, w_up, w_down))
        return tuple(adamw(ss, g, (w_gate, w_up, w_down), (m_gate, m_up, m_down), (v_gate, v_up, v_down)))

    return jax.shard_map(
        step,
        mesh=mesh,
        in_specs=(P(("rep", "dp")),) * 2 + (P(),) * 9,
        out_specs=(P("rep"),) * 9,
        check_vma=False,
    )
```
